256 devices in a mesh: line: 8 (over y, x_hi), surf: 32 (over z, x_lo, core).
Axes of the slice: x: 4 (x_hi: 2, x_lo: 2; x = x_hi * 2 + x_lo), y: 4, z: 8, core: 2. Of those that a mesh axis runs over, the one named last changes fastest.
Arguments:
- face_coef: float32 [32, 4096], P('line', 'surf'), may hold values from 0.5 to 2
- face_mix: float32 [32, 17, 17, 4096], P('line', None, None, 'surf'), may hold values from -0.6 to 0.6
- cell_mix: float32 [32, 17, 17, 4096], P('line', None, None, 'surf'), may hold values from -0.6 to 0.6
- time_term: float32 [32, 17, 4096], P('line', None, 'surf'), may hold values from 0.0005 to 1
- couple: float32 [32, 4, 17, 4096], P('line', None, None, 'surf'), may hold values from 0.0005 to 0.05
- rhs: float32 [32, 17, 4096], P('line', None, 'surf'), may hold values from -0.4 to 0.4
- start_delta: float32 [32, 17, 4096], P('line', None, 'surf'), may hold values from -6 to 6
- neighbours: int32 [4, 4096], P(None, 'surf'), may hold values from -1 to 4095, as said below
- wall_type: int32 [4096], P('surf'), may hold values from 0 to 2
Outputs:
- delta: float32 [32, 17, 4096], P('line', None, 'surf')
The draws below stay inside these ranges and needn't reach their ends.
Inputs may be any that keep to these rules, and one draw needn't show every extreme that they name: `neighbours`: -1 marks a missing neighbour. Entries 0 and 1 of a line are -1 or lines of its own grid block (blocks are the aligned runs of 128 lines). Entry 2 is a line of its own block or one of the last 16 lines of the block before it; entry 3 a line of its own block or one of the first 16 lines of the block after it; blocks follow one another cyclically. A line is the neighbour of its neighbour. `wall_type`: 0 slip wall, 1 isothermal wall, 2 catalytic wall.
All inputs are finite; a program needn't handle non-finite values.
Results may differ from the reference program's by a relative error of at most 0.0003.
Values sent between devices are 32-bit elements; how exact they have to be, the bound alone decides.
No kernel may reach another device: no remote copies, remote signals or barrier semaphores. Data moves between devices by JAX's collectives and lax.ppermute only.
A program may use at most 64 MiB of HBM per device.

```python
import math
import jax
import jax.numpy as jnp
from jax import lax

NS = 17
BLOCK = 128
COLS = 16
ITERS = 2
NC = 32
LINES = 4096


def draw_neighbours(key, part):
    line_total = LINES
    block_count = LINES // BLOCK
    row_count = BLOCK // COLS
    flips = jax.random.randint(jax.random.fold_in(key, 17), (block_count,), 0, 2)
    global_line = jnp.arange(line_total, dtype=jnp.int32)
    block_of = global_line // BLOCK
    within = global_line % BLOCK
    row_of = within // COLS
    column = within % COLS
    before = jnp.where(column > 0, global_line - 1, -1)
    after = jnp.where(column < COLS - 1, global_line + 1, -1)
    block_prev = (block_of - 1) % block_count
    column_prev = jnp.where(flips[block_prev] == 1, COLS - 1 - column, column)
    down_line = jnp.where(row_of > 0, global_line - COLS, block_prev * BLOCK + (row_count - 1) * COLS + column_prev)
    block_next = (block_of + 1) % block_count
    column_next = jnp.where(flips[block_of] == 1, COLS - 1 - column, column)
    up_line = jnp.where(row_of < row_count - 1, global_line + COLS, block_next * BLOCK + column_next)
    return jnp.stack([before, after, down_line, up_line]).astype(jnp.int32)


def touch_ends(values, own_key, smallest, top_value):
    spot = [jax.random.randint(jax.random.fold_in(own_key, axis), (), 0, length) for axis, length in enumerate(values.shape)]
    widest = values.shape.index(max(values.shape))
    beside = spot[:widest] + [(spot[widest] + 1) % values.shape[widest]] + spot[widest + 1:]
    return values.at[tuple(spot)].set(smallest).at[tuple(beside)].set(top_value)


def block_levels(stream_key, dims, split, least, high):
    level, own = 1.0, jax.random.fold_in(stream_key, 6)
    for position, parts in split:
        steps = jnp.exp(jax.random.uniform(jax.random.fold_in(own, position), (parts,), jnp.float32, least / len(split), high / len(split)))
        level = level * jnp.repeat(steps, dims[position] // parts).reshape([-1 if axis == position else 1 for axis in range(len(dims))])
    return level


def normal_values(key, extent, deviation, limit, shards=(), held_as=jnp.bfloat16):
    level = block_levels(key, extent, shards, -0.22, 0.18) if shards else 1.0
    values = jax.random.normal(key, extent, jnp.float32) * deviation * level
    return jnp.minimum(jnp.maximum(values, -limit), limit).astype(held_as)


def setup_inputs(seed: int = 0) -> dict:
    arg_keys = jax.random.split(jax.random.key(seed), 10)
    face_coef = jnp.clip(jnp.exp(math.log(2.0) - 1.3862944 * jax.random.uniform(arg_keys[0], (NC, LINES), jnp.float32) ** block_levels(arg_keys[0], (NC, LINES), ((0, 8), (1, 32)), -0.2, 0.2)), 0.5, 2.0)
    face_mix = normal_values(arg_keys[1], (NC, NS, NS, LINES), 0.1, 0.6, ((0, 8), (3, 32)), jnp.float32)
    cell_mix = normal_values(arg_keys[2], (NC, NS, NS, LINES), 0.1, 0.6, ((0, 8), (3, 32)), jnp.float32)
    time_term = jnp.clip(jnp.exp(math.log(1.0) - 7.6009024 * jax.random.uniform(arg_keys[3], (NC, NS, LINES), jnp.float32) ** block_levels(arg_keys[3], (NC, NS, LINES), ((0, 8), (2, 32)), -0.2, 0.2)), 0.0005, 1.0)
    couple = jnp.clip(jnp.exp(math.log(0.05) - 4.6051702 * jax.random.uniform(arg_keys[4], (NC, 4, NS, LINES), jnp.float32) ** block_levels(arg_keys[4], (NC, 4, NS, LINES), ((0, 8), (3, 32)), -0.2, 0.2)), 0.0005, 0.05)
    rhs = normal_values(arg_keys[5], (NC, NS, LINES), 0.05, 0.4, ((0, 8), (2, 32)), jnp.float32)
    start_delta = normal_values(arg_keys[6], (NC, NS, LINES), 1.0, 6.0, ((0, 8), (2, 32)), jnp.float32)
    neighbours = draw_neighbours(jax.random.fold_in(arg_keys[9], 71), 0)
    wall_type = touch_ends(jax.random.randint(arg_keys[8], (LINES,), 0, 3), jax.random.fold_in(arg_keys[8], 1), 0, 2).astype(jnp.int32)
    return dict(face_coef=face_coef, face_mix=face_mix, cell_mix=cell_mix, time_term=time_term, couple=couple, rhs=rhs, start_delta=start_delta, neighbours=neighbours, wall_type=wall_type)


wall_levels = (0.5, 4.0, 32.0)

def matrix_product(matrix_left, matrix_right):
    return jnp.einsum('ijb,jkb->ikb', matrix_left, matrix_right, precision=lax.Precision.HIGHEST)

def matrix_vector(matrix_left, vector_right):
    return jnp.einsum('ijb,jb->ib', matrix_left, vector_right, precision=lax.Precision.HIGHEST)

def solve_lines(face_part, mix_part, cell_part, extra_part, wall_part, source_part):
    width = mix_part.shape[1]
    identity = jnp.eye(width, dtype=jnp.float32)[:, :, None]
    coef_below = jnp.concatenate([wall_part[None], face_part[:-1]], 0)
    mix_below = jnp.concatenate([jnp.zeros_like(mix_part[:1]), mix_part[:-1]], 0)
    lower_mask = (jnp.arange(face_part.shape[0]) > 0).astype(jnp.float32)

    def forward_step(state_prev, inputs):
        coupler_prev, solved_prev = state_prev
        coef_up, coef_down, mix_up, mix_down, mix_cell, extra, source, lower_on = inputs
        diagonal = identity * extra[None] + (coef_up + coef_down)[None, None] * identity + mix_cell - jnp.swapaxes(mix_cell, 0, 1)
        lower = lower_on * (-coef_down[None, None] * identity - jnp.swapaxes(mix_down, 0, 1))
        upper = -coef_up[None, None] * identity + mix_up
        schur = diagonal - matrix_product(lower, coupler_prev)
        stacked = jnp.concatenate([upper, (source - matrix_vector(lower, solved_prev))[:, None]], axis=1)
        solved = jnp.linalg.solve(jnp.moveaxis(schur, -1, 0), jnp.moveaxis(stacked, -1, 0))
        solved = jnp.moveaxis(solved, 0, -1)
        coupler_now = solved[:, :width]
        vector_now = solved[:, width]
        return ((coupler_now, vector_now), (coupler_now, vector_now))
    lines_here = source_part.shape[-1]
    zero_matrix = jnp.zeros((width, width, lines_here), jnp.float32)
    zero_vector = jnp.zeros((width, lines_here), jnp.float32)
    inputs = (face_part, coef_below, mix_part, mix_below, cell_part, extra_part, source_part, lower_mask)
    _, (couplers, forward) = lax.scan(forward_step, (zero_matrix, zero_vector), inputs)

    def back_step(above, inputs):
        coupler, vector = inputs
        result = vector - matrix_vector(coupler, above)
        return (result, result)
    _, solution = lax.scan(back_step, zero_vector, (couplers, forward), reverse=True)
    return solution

def reference(face_coef, face_mix, cell_mix, time_term, couple, rhs, start_delta, neighbours, wall_type):
    line_total = rhs.shape[2]
    block_count = line_total // BLOCK
    wall_term = jnp.zeros(wall_type.shape, jnp.float32)
    for wall_kind, wall_value in enumerate(wall_levels):
        wall_term = wall_term + jnp.where(wall_type == wall_kind, wall_value, 0.0).astype(jnp.float32)
    valid_mask = (neighbours >= 0).astype(jnp.float32)
    safe_index = jnp.where(neighbours >= 0, neighbours, 0).astype(jnp.int32)
    diag_extra = time_term + jnp.sum(couple, axis=1)
    weights = couple * valid_mask[None, :, None, :]

    def sweep_once(previous):
        neighbour_vals = jnp.take(previous, safe_index, axis=2)
        right_side = rhs + jnp.sum(weights * jnp.swapaxes(neighbour_vals, 1, 2), axis=1)

        def one_block(block_number):
            start = (block_number * BLOCK).astype(jnp.int32)
            pieces = [lax.dynamic_slice_in_dim(array, start, BLOCK, axis=array.ndim - 1) for array in (face_coef, face_mix, cell_mix, diag_extra, wall_term, right_side)]
            return solve_lines(*pieces)
        solved = lax.map(one_block, jnp.arange(block_count, dtype=jnp.int32))
        return jnp.moveaxis(solved, 0, 2).reshape(right_side.shape)
    previous = start_delta
    for sweep_number in range(ITERS):
        previous = sweep_once(previous)
    return previous
```

```python
import jax
import jax.numpy as jnp
from jax import lax
from jax.experimental import pallas as pl
from jax.experimental.pallas import tpu as pltpu
from jax.sharding import PartitionSpec as P

COLS = 16
WIDTH = 17
GROUPS = 8
LANES = 128
DROWS = 24 * WIDTH
BROWS = 40 * WIDTH
BELOWROWS = 296
VROWS = 72
MATRIX_GROUPS = 43
TOTALROWS = 64 * (MATRIX_GROUPS + 2)
CELL_AT, TIME_AT, RHS_AT, COUPLE_AT, COEF_AT, RIGHT_AT = 1160, 2320, 2392, 2464, 2736, 2752
WALLS = (0.5, 4.0, 32.0)
FP = jnp.float32


def lane_ids(rows):
    return lax.broadcasted_iota(jnp.int32, (rows, LANES), 1)


def sub_ids(rows):
    return lax.broadcasted_iota(jnp.int32, (rows, LANES), 0)


def swap_blocks(regs):
    lanes = lane_ids(8)
    for k in (1, 2, 4):
        high = (lanes // (COLS * k)) % 2 == 1
        result = list(regs)
        for a in range(8):
            if a & k:
                continue
            b = a | k
            result[a] = jnp.where(high, pltpu.roll(regs[b], COLS * k, 1), regs[a])
            result[b] = jnp.where(high, regs[b], pltpu.roll(regs[a], LANES - COLS * k, 1))
        regs = result
    return regs


def row(ref, at):
    return ref[pl.ds(at, 1), :]


def tile(ref, at):
    return ref[pl.ds(at, 8), :]


def strided(ref, at, stride):
    return ref[pl.ds(at, 8, stride=stride), :]


def along(value, lanes):
    rows = value.shape[0]
    value, lanes = jnp.broadcast_to(value, (8, LANES)), jnp.broadcast_to(lanes, (8, LANES))
    return jnp.take_along_axis(value, lanes, axis=1, mode="promise_in_bounds")[:rows]


def pack_kernel(coef_ref, face_ref, cell_ref, time_ref, couple_ref, rhs_ref, out_ref, stage):
    pieces = []
    for ref in (face_ref, cell_ref, time_ref, rhs_ref, couple_ref, coef_ref):
        rows = ref.size // LANES
        flat = ref if len(ref.shape) == 2 else ref.reshape(rows, LANES)
        for at in range(0, rows - 7, 8):
            pieces.append((flat, at))
        if rows % 8:
            spot = 8 * len([p for p in pieces if p[0] is stage])
            stage[pl.ds(spot, 8), :] = jnp.zeros((8, LANES), FP)
            stage[pl.ds(spot, rows % 8), :] = flat[pl.ds(rows - rows % 8, rows % 8), :]
            pieces.append((stage, spot))
    zeros = jnp.zeros((8, LANES), FP)
    for g in range(MATRIX_GROUPS):
        regs = []
        for w in range(8):
            n = 8 * g + w
            regs.append(tile(*pieces[n]) if n < len(pieces) else zeros)
        regs = swap_blocks(regs)
        for d in range(8):
            out_ref[d, pl.ds(8 * g, 8), :] = regs[d]


def right_kernel(
    start_ref, low_ref, high_ref, index_ref, from_ref, couple_ref, rhs_ref, _, out_ref, stage, sem,
):
    start, low, high, rhs = [ref.reshape(4 * WIDTH, LANES) for ref in (start_ref, low_ref, high_ref, rhs_ref)]
    couple = couple_ref.reshape(16 * WIDTH, LANES)
    ids = sub_ids(8)
    lanes = [jnp.broadcast_to(index_ref[pl.ds(n, 1), :], (8, LANES)) for n in range(4)]
    kinds = [jnp.broadcast_to(from_ref[pl.ds(n, 1), :], (8, LANES)) for n in range(4)]

    def total(load, weight):
        value = load(rhs)
        sources = [load(ref) for ref in (start, low, high)]
        for n in range(4):
            got = jnp.zeros((8, LANES), FP)
            for d, source in enumerate(sources):
                got = jnp.where(kinds[n] == d, along(source, lanes[n]), got)
            value = value + weight(n) * got
        return value

    regs = []
    for c in range(4):
        for h in range(2):
            regs.append(total(
                lambda ref: strided(ref, 32 * h + c, 4),
                lambda n: strided(couple, (17 * c + 8 * h) * 4 + n, 4),
            ))

    def last_weight(n):
        value = jnp.zeros((8, LANES), FP)
        for c in range(4):
            value = jnp.where(ids == 4 + c, row(couple, (17 * c + 16) * 4 + n), value)
        return value

    regs.append(total(lambda ref: tile(ref, 60), last_weight))
    zeros = jnp.zeros((8, LANES), FP)
    for g in range(2):
        part = swap_blocks((regs + [zeros] * 7)[8 * g : 8 * g + 8])
        for d in range(8):
            stage[d, pl.ds(8 * g, 8), :] = part[d]
    copy = pltpu.make_async_copy(stage, out_ref.at[:, pl.ds(8 * MATRIX_GROUPS, 16), :], sem)
    copy.start()
    copy.wait()


def left_at(j):
    return j if j < 16 else 32


def right_at(j):
    return 16 + j if j < 16 else 33


def invert_in_place(refs):
    ids = sub_ids(8)
    for k in range(WIDTH):
        for ref, base in refs:
            pivot = jnp.broadcast_to(1.0 / row(ref, base + 24 * k + k), (8, LANES))
            scaled = [tile(ref, base + 24 * k + 8 * v) * pivot for v in range(3)]
            here = ids == k % 8
            scaled[k // 8] = jnp.where(here, pivot, scaled[k // 8])
            for i in range(WIDTH):
                if i == k:
                    continue
                factor = row(ref, base + 24 * i + k)
                for v in range(3):
                    old = tile(ref, base + 24 * i + 8 * v)
                    if v == k // 8:
                        old = jnp.where(here, 0.0, old)
                    ref[pl.ds(base + 24 * i + 8 * v, 8), :] = old - factor * scaled[v]
            for v in range(3):
                ref[pl.ds(base + 24 * k + 8 * v, 8), :] = scaled[v]


def normalise(inverse, inverse_base, source, source_base, result, result_base):
    def step(i, _):
        at = pl.multiple_of(24 * i, 8)
        sums = [None] * 5
        for j in range(WIDTH):
            factor = row(inverse, inverse_base + at + j)
            for v in range(5):
                term = factor * tile(source, source_base + 40 * j + 8 * v)
                sums[v] = term if j == 0 else sums[v] + term
        to = pl.multiple_of(40 * i, 8)
        for v in range(5):
            result[pl.ds(result_base + to + 8 * v, 8), :] = sums[v]
        return 0

    lax.fori_loop(0, WIDTH, step, 0)


def eliminate(blocks, base, diag, diag_base, low, low_base, high, high_base, new, new_base, new_diag, new_diag_base):
    ids = sub_ids(8)

    def step(i, _):
        at = pl.multiple_of(40 * i, 8)
        first, second = [None] * 5, [None] * 5
        for j in range(WIDTH):
            below = row(blocks, base + at + left_at(j))
            above = row(blocks, base + at + right_at(j))
            for v in range(5):
                term = below * tile(low, low_base + 40 * j + 8 * v)
                first[v] = term if j == 0 else first[v] + term
                term = above * tile(high, high_base + 40 * j + 8 * v)
                second[v] = term if j == 0 else second[v] + term
        for v in range(2):
            new[pl.ds(new_base + at + 8 * v, 8), :] = -first[v]
            new[pl.ds(new_base + at + 16 + 8 * v, 8), :] = -second[2 + v]
        rest = tile(blocks, base + at + 32) - first[4] - second[4]
        rest = jnp.where(ids == 0, -first[4], jnp.where(ids == 1, -second[4], rest))
        new[pl.ds(new_base + at + 32, 8), :] = rest
        to = pl.multiple_of(24 * i, 8)
        for v in range(2):
            new_diag[pl.ds(new_diag_base + to + 8 * v, 8), :] = (
                tile(diag, diag_base + to + 8 * v) - first[2 + v] - second[v]
            )
        new_diag[pl.ds(new_diag_base + to + 16, 8), :] = (
            tile(diag, diag_base + to + 16) - pltpu.roll(first[4], 7, 0) - second[4]
        )
        return 0

    lax.fori_loop(0, WIDTH, step, 0)


def matvec(ref, base, stride, at, value_row):
    sums = [None] * 3
    for j in range(WIDTH):
        value = value_row(j)
        here = at(j)
        for h in range(2):
            term = strided(ref, base + 8 * h * stride + here, stride) * value
            sums[h] = term if j == 0 else sums[h] + term
        term = row(ref, base + 16 * stride + here) * value
        sums[2] = term if j == 0 else sums[2] + term
    return sums


def minus(a, b):
    return [x - y for x, y in zip(a, b)]


def plain(j):
    return j


def vector_of(ref, base, last):
    return [tile(ref, base), tile(ref, base + 8), row(ref, last)]


def put_vector(ref, base, last, value):
    ref[pl.ds(base, 8), :] = value[0]
    ref[pl.ds(base + 8, 8), :] = value[1]
    ref[pl.ds(last, 1), :] = value[2]


def moved(value, steps):
    return [pltpu.roll(x, (COLS * steps) % LANES, 1) for x in value]


class Scratch:
    def __init__(self, ref):
        self.ref, self.next = ref, 0

    def hold(self, value):
        base = 24 * self.next
        self.next += 1
        put_vector(self.ref, base, base + 16, value)
        return lambda j: row(self.ref, base + j)


def back_substitute(held, scratch, top, forward):
    below = scratch.hold(moved(top, 1))
    own = scratch.hold(top)

    def part(index, low, high):
        base = index * BROWS
        value = minus(forward[index], matvec(held, base, 40, left_at, low))
        return minus(value, matvec(held, base, 40, right_at, high))

    one = part(2, below, own)
    one_rows = scratch.hold(one)
    return [part(0, below, one_rows), one, part(1, one_rows, own), top]


def put_cells(ref, cells, copies):
    for c in range(4):
        for d in range(copies):
            for h in range(2):
                ref[d, pl.ds(16 * c + 8 * h, 8), :] = cells[c][h]
            ref[d, pl.ds(64 + c, 1), :] = cells[c][2]
    for d in range(copies):
        ref[d, pl.ds(68, 4), :] = jnp.zeros((4, LANES), FP)


def factor_kernel(
    got_ref, wall_ref, solved_ref, inverse_ref, blocks_ref, held_ref, vectors_ref,
    stage, below, work_blocks, work_diag, low, high, scratch_ref,
):
    groups = lane_ids(1) // COLS
    for g in range(TOTALROWS // 64):
        regs = swap_blocks([got_ref[d, pl.ds(8 * g, 8), :] for d in range(8)])
        for w in range(8):
            stage[pl.ds(64 * g + 8 * w, 8), :] = regs[w]
    for c in range(4):
        for piece in range(5):
            at, step = (RHS_AT + c, 4) if piece == 0 else (COUPLE_AT + 68 * c + piece - 1, 4)
            for h in range(2):
                vectors_ref[pl.ds(VROWS * piece + 16 * c + 8 * h, 8), :] = strided(stage, at + 32 * h, step)
            vectors_ref[pl.ds(VROWS * piece + 64 + c, 1), :] = row(stage, at + 64)
    for piece in range(5):
        vectors_ref[pl.ds(VROWS * piece + 68, 4), :] = jnp.zeros((4, LANES), FP)
    has_below = jnp.where(groups == 0, 0.0, 1.0)
    has_above = jnp.where(groups == GROUPS - 1, 0.0, 1.0)
    for i in range(WIDTH):
        for h in range(2):
            value = strided(stage, 4 * (17 * i + 8 * h) + 3, 4)
            below[pl.ds(17 * i + 8 * h, 8), :] = pltpu.roll(value, COLS, 1) * has_below
    for i in range(0, WIDTH, 8):
        if i < 16:
            value = strided(stage, 4 * (17 * i + 16) + 3, 68)
            below[pl.ds(17 * i + 16, 8, stride=17), :] = pltpu.roll(value, COLS, 1) * has_below
    for at, source in ((288, 4 * 288 + 3), (289, COEF_AT + 3)):
        value = jnp.broadcast_to(row(stage, source), (8, LANES))
        below[pl.ds(at, 1), :] = (pltpu.roll(value, COLS, 1) * has_below)[:1]
    wall = jnp.zeros((1, LANES), FP)
    for kind, level in enumerate(WALLS):
        wall = wall + jnp.where(wall_ref[...] == kind, level, 0.0)
    ids = sub_ids(8)

    def build(c, blocks, blocks_base, diag, diag_base):
        lower, scale, shift = (below, 1, 0) if c == 0 else (stage, 4, c - 1)
        coef_low = row(below, 289) if c == 0 else row(stage, COEF_AT + c - 1)
        coef_up = row(stage, COEF_AT + c)
        on_diag = coef_low + coef_up
        if c == 0:
            on_diag = on_diag + wall * (1.0 - has_below)
        keep = has_above if c == 3 else None

        def up(value):
            return value if keep is None else value * keep

        def at(i, j):
            return 4 * (17 * i + j) + c

        def lower_at(i, j):
            return scale * (17 * i + j) + shift

        for i in range(WIDTH):
            extra = on_diag + row(stage, TIME_AT + 4 * i + c)
            for n in range(4):
                extra = extra + row(stage, COUPLE_AT + 68 * c + 4 * i + n)
            for h in range(2):
                down = -strided(lower, lower_at(8 * h, i), 17 * scale)
                entry = strided(stage, CELL_AT + at(i, 8 * h), 4) - strided(stage, CELL_AT + at(8 * h, i), 68)
                face = strided(stage, at(i, 8 * h), 4)
                if i // 8 == h:
                    here = ids == i % 8
                    entry = entry + jnp.where(here, extra, 0.0)
                    face = face - jnp.where(here, coef_up, 0.0)
                    down = down - jnp.where(here, coef_low, 0.0)
                diag[pl.ds(diag_base + 24 * i + 8 * h, 8), :] = entry
                blocks[pl.ds(blocks_base + 40 * i + 8 * h, 8), :] = down
                blocks[pl.ds(blocks_base + 40 * i + 16 + 8 * h, 8), :] = up(face)
            side = -row(lower, lower_at(16, i))
            face = row(stage, at(i, 16))
            if i < 16:
                corner = row(stage, CELL_AT + at(i, 16)) - row(stage, CELL_AT + at(16, i))
            else:
                corner, side, face = extra, side - coef_low, face - coef_up
            value = row(stage, RIGHT_AT + (16 * c + i if i < 16 else 68 + c))
            packed = jnp.where(ids == 0, side, jnp.where(ids == 1, up(face), jnp.where(ids == 2, value, 0.0)))
            blocks[pl.ds(blocks_base + 40 * i + 32, 8), :] = packed
            diag[pl.ds(diag_base + 24 * i + 16, 8), :] = jnp.where(ids == 0, corner, 0.0)

    B, D = BROWS, DROWS
    build(0, work_blocks, 0, inverse_ref, 0)
    build(2, work_blocks, B, inverse_ref, D)
    build(1, blocks_ref, 0, work_diag, 0)
    build(3, blocks_ref, B, work_diag, D)
    invert_in_place([(inverse_ref, 0), (inverse_ref, D)])
    normalise(inverse_ref, 0, work_blocks, 0, held_ref, 0)
    normalise(inverse_ref, D, work_blocks, B, held_ref, B)

    def turn(source, source_base, result, steps):
        for t in range(BROWS // 8):
            result[pl.ds(8 * t, 8), :] = pltpu.roll(
                tile(source, source_base + 8 * t), (COLS * steps) % LANES, 1
            )

    turn(held_ref, 0, high, -1)
    eliminate(blocks_ref, 0, work_diag, 0, held_ref, 0, held_ref, B, work_blocks, 0, inverse_ref, 2 * D)
    eliminate(blocks_ref, B, work_diag, D, held_ref, B, high, 0, blocks_ref, 2 * B, work_diag, 0)
    invert_in_place([(inverse_ref, 2 * D)])
    normalise(inverse_ref, 2 * D, work_blocks, 0, held_ref, 2 * B)
    turn(held_ref, 2 * B, high, -1)
    eliminate(
        blocks_ref, 2 * B, work_diag, 0, held_ref, 2 * B, high, 0, blocks_ref, 3 * B, inverse_ref, 3 * D
    )
    for k in range(3):
        source = 3 + k
        work_diag[pl.ds(0, D), :] = inverse_ref[pl.ds(source * D, D), :]
        invert_in_place([(inverse_ref, source * D)])
        normalise(inverse_ref, source * D, blocks_ref, source * B, work_blocks, 0)
        turn(work_blocks, 0, low, 2**k)
        turn(work_blocks, 0, high, -(2**k))
        if k < 2:
            new, new_base = blocks_ref, (source + 1) * B
        else:
            new, new_base = work_blocks, B
        eliminate(
            blocks_ref, source * B, work_diag, 0, low, 0, high, 0, new, new_base, inverse_ref, (source + 1) * D
        )
    invert_in_place([(inverse_ref, 6 * D)])
    scratch = Scratch(scratch_ref)
    last = matvec(inverse_ref, 6 * D, 24, plain, lambda j: row(work_blocks, B + 40 * j + 34))
    forward = []
    for index in range(3):
        base = index * B
        forward.append([
            strided(held_ref, base + 34, 40),
            strided(held_ref, base + 320 + 34, 40),
            row(held_ref, base + 640 + 34),
        ])
    put_cells(solved_ref, back_substitute(held_ref, scratch, last, forward), GROUPS)


def solve_kernel(
    all_ref, low_ref, high_ref, index_ref, from_ref, vectors_ref, inverse_ref, blocks_ref, held_ref,
    out_ref, right, scratch_ref,
):
    for t in range(VROWS // 8):
        at = 8 * t
        total = tile(vectors_ref, at)
        for n in range(4):
            lanes = jnp.broadcast_to(index_ref[pl.ds(n, 1), :], (8, LANES))
            source = jnp.broadcast_to(from_ref[pl.ds(n, 1), :], (8, LANES))
            value = jnp.zeros((8, LANES), FP)
            for d in range(GROUPS + 2):
                if d < GROUPS:
                    got = all_ref[d, pl.ds(at, 8), :]
                else:
                    got = tile(low_ref if d == GROUPS else high_ref, at)
                value = jnp.where(source == d, along(got, lanes), value)
            total = total + tile(vectors_ref, VROWS * (n + 1) + at) * value
        right[pl.ds(at, 8), :] = total
    B, D = BROWS, DROWS
    scratch = Scratch(scratch_ref)

    def cell_rows(c):
        return lambda j: row(right, 16 * c + j if j < 16 else 64 + c)

    def cell(c):
        return vector_of(right, 16 * c, 64 + c)

    def apply(index, rows):
        return matvec(inverse_ref, index * D, 24, plain, rows)

    def reduce(value, index, low, high):
        value = minus(value, matvec(blocks_ref, index * B, 40, left_at, low))
        return minus(value, matvec(blocks_ref, index * B, 40, right_at, high))

    zero = apply(0, cell_rows(0))
    two = apply(1, cell_rows(2))
    zero_rows, two_rows = scratch.hold(zero), scratch.hold(two)
    next_zero = scratch.hold(moved(zero, -1))
    one = apply(2, scratch.hold(reduce(cell(1), 0, zero_rows, two_rows)))
    three = reduce(cell(3), 1, two_rows, next_zero)
    one_rows, next_one = scratch.hold(one), scratch.hold(moved(one, -1))
    three = reduce(three, 2, one_rows, next_one)
    for k in range(3):
        scaled = apply(3 + k, scratch.hold(three))
        low, high = scratch.hold(moved(scaled, 2**k)), scratch.hold(moved(scaled, -(2**k)))
        three = reduce(three, 3 + k, low, high)
    last = apply(6, scratch.hold(three))
    cells = back_substitute(held_ref, scratch, last, [zero, two, one])
    for g in range(2):
        regs = []
        for w in range(8):
            v = 8 * g + w
            if v < 8:
                regs.append(cells[v // 2][v % 2])
            elif v == 8:
                ids = sub_ids(8)
                value = jnp.zeros((8, LANES), FP)
                for c in range(4):
                    value = jnp.where(ids == c, cells[c][2], value)
                regs.append(value)
            else:
                regs.append(jnp.zeros((8, LANES), FP))
        regs = swap_blocks(regs)
        for d in range(8):
            out_ref[d, pl.ds(8 * g, 8), :] = regs[d]


def unpack_kernel(got_ref, out_ref):
    flat = out_ref.reshape(4 * WIDTH, LANES)
    for g in range(2):
        regs = swap_blocks([got_ref[d, pl.ds(8 * g, 8), :] for d in range(8)])
        if g == 0:
            for c in range(4):
                for h in range(2):
                    flat[pl.ds(32 * h + c, 8, stride=4), :] = regs[2 * c + h]
        else:
            flat[pl.ds(64, 4), :] = regs[0][:4]


def edge_kernel(top_ref, bottom_ref, top_out_ref, bottom_out_ref):
    top_out_ref[...] = top_ref[0]
    bottom_out_ref[...] = bottom_ref[0]


def shape(*dims):
    return jax.ShapeDtypeStruct(dims, FP)


def call(kernel, outputs, scratch, args, flops, name, limit=16, **more):
    return pl.pallas_call(
        kernel,
        out_shape=outputs,
        scratch_shapes=[pltpu.VMEM(dims, FP) if isinstance(dims, tuple) else dims for dims in scratch],
        compiler_params=pltpu.CompilerParams(vmem_limit_bytes=limit * 2**20),
        cost_estimate=pl.CostEstimate(flops=flops, bytes_accessed=1000000, transcendentals=0),
        name=name,
        **more,
    )(*args)


def across(value):
    return lax.all_to_all(value, "line", 0, 0, tiled=True)


def on_device(
    face_coef, face_mix, cell_mix, time_term, couple, rhs, start_delta, neighbours, wall_type
):
    count = lax.axis_size("surf")
    up = [(i, (i + 1) % count) for i in range(count)]
    down = [(target, source) for source, target in up]
    lines = wall_type.shape[0]
    place = lax.axis_index("line")
    start = start_delta.transpose(1, 0, 2)
    rhs_rows = rhs.transpose(1, 0, 2)
    couple_rows = couple.transpose(0, 2, 1, 3).reshape(4 * WIDTH, 4, lines)
    face, cell = [a.transpose(1, 2, 0, 3).reshape(WIDTH * WIDTH, 4, lines) for a in (face_mix, cell_mix)]
    low = lax.ppermute(start, "surf", up)
    high = lax.ppermute(start, "surf", down)

    surf_place = lax.axis_index("surf")
    local = (neighbours - (surf_place * lines - COLS)) % (lines * count)
    is_low = local < COLS
    is_own = (local >= COLS) & (local < COLS + lines)
    valid = neighbours >= 0
    own_index = jnp.clip(local - COLS, 0, lines - 1)
    kind = jnp.where(is_own, 0, jnp.where(is_low, 1, 2))
    kind = jnp.where(valid, kind, -1)
    index = jnp.where(is_own, own_index, jnp.where(is_low, local + lines - COLS, local - lines - COLS))
    index = jnp.clip(index, 0, lines - 1)
    source = jnp.where(is_own, own_index // COLS, jnp.where(is_low, GROUPS, GROUPS + 1))
    source = jnp.where(valid, source, -1)
    offset = index % COLS

    def for_group(array):
        mine = lax.dynamic_slice_in_dim(array, place * COLS, COLS, axis=array.ndim - 1)
        return jnp.tile(mine, (1, GROUPS))

    group_offset = for_group(offset) + (jnp.arange(lines, dtype=jnp.int32) // COLS * COLS)[None]
    group_source = for_group(source)
    group_wall = for_group(wall_type[None])

    packed = call(
        pack_kernel,
        shape(GROUPS, TOTALROWS // 8, LANES),
        [(40, LANES)],
        (face_coef, face, cell, time_term.transpose(1, 0, 2), couple_rows, rhs_rows),
        20000000,
        "pack",
    )
    any_place = pl.BlockSpec(memory_space=pl.ANY)
    packed = call(
        right_kernel,
        shape(GROUPS, TOTALROWS // 8, LANES),
        [(GROUPS, 16, LANES), pltpu.SemaphoreType.DMA(())],
        (start, low, high, index, kind, couple_rows, rhs_rows, packed),
        1000000,
        "right",
        in_specs=[pl.BlockSpec(memory_space=pltpu.VMEM)] * 7 + [any_place],
        out_specs=any_place,
        input_output_aliases={7: 0},
    )
    packed, group_offset, group_source, group_wall = lax.optimization_barrier(
        (packed, group_offset, group_source, group_wall)
    )
    received = across(packed)
    solved, inverses, blocks, held, vectors = call(
        factor_kernel,
        (
            shape(GROUPS, VROWS, LANES),
            shape(7 * DROWS, LANES),
            shape(6 * BROWS, LANES),
            shape(3 * BROWS, LANES),
            shape(5 * VROWS, LANES),
        ),
        [
            (TOTALROWS, LANES), (BELOWROWS, LANES), (2 * BROWS, LANES), (2 * DROWS, LANES),
            (BROWS, LANES), (BROWS, LANES), (24 * 4, LANES),
        ],
        (received, group_wall),
        30000000,
        "factor",
    )
    everyone = across(solved)
    top, bottom = call(
        edge_kernel, (shape(VROWS, LANES), shape(VROWS, LANES)), [], (everyone, everyone), 1000, "edge", 1,
        grid=(1,),
        in_specs=[pl.BlockSpec((1, VROWS, LANES), lambda i: (GROUPS - 1, 0, 0)), pl.BlockSpec((1, VROWS, LANES), lambda i: (0, 0, 0))],
    )
    low = lax.ppermute(top, "surf", up)
    high = lax.ppermute(bottom, "surf", down)
    sent = call(
        solve_kernel,
        shape(GROUPS, 16, LANES),
        [(VROWS, LANES), (24 * 24, LANES)],
        (everyone, low, high, group_offset, group_source, vectors, inverses, blocks, held),
        3000000,
        "solve",
    )
    done = call(unpack_kernel, shape(WIDTH, 4, LANES), [], (across(sent),), 100000, "unpack")
    return done.transpose(1, 0, 2)


def solution(mesh):
    placed = (
        P("line", "surf"),
        P("line", None, None, "surf"),
        P("line", None, None, "surf"),
        P("line", None, "surf"),
        P("line", None, None, "surf"),
        P("line", None, "surf"),
        P("line", None, "surf"),
        P(None, "surf"),
        P("surf"),
    )
    return jax.shard_map(
        on_device, mesh=mesh, in_specs=placed, out_specs=P("line", None, "surf"), check_vma=False
    )
```

```python
import jax
import jax.numpy as jnp
from jax import lax
from jax.experimental import pallas as pl
from jax.experimental.pallas import tpu as pltpu
from jax.sharding import PartitionSpec as P

COLS = 16
WIDTH = 17
GROUPS = 8
LANES = 128
DROWS = 24 * WIDTH
BROWS = 40 * WIDTH
BELOWROWS = 296
VROWS = 72
MATRIX_BLOCKS = 17
TOTALROWS = 128 * (MATRIX_BLOCKS + 1)
SKEW_TILES = WIDTH * (WIDTH - 1) // 2
SKEW_AT = 1160
TIME_AT = SKEW_AT + 4 * SKEW_TILES
RHS_AT, COUPLE_AT = TIME_AT + 72, TIME_AT + 144
COEF_AT = COUPLE_AT + 272
RIGHT_AT = 128 * MATRIX_BLOCKS
WALLS = (0.5, 4.0, 32.0)
FP = jnp.float32


def lane_ids(rows):
    return lax.broadcasted_iota(jnp.int32, (rows, LANES), 1)


def sub_ids(rows):
    return lax.broadcasted_iota(jnp.int32, (rows, LANES), 0)


def skew_tile(i, j):
    return 16 * i - i * (i - 1) // 2 + j - i - 1


def split_lines(tiles, out_ref, at):
    turned = jnp.concatenate(tiles, axis=0).T
    for d in range(GROUPS):
        out_ref[d, pl.ds(at, COLS), :] = turned[COLS * d : COLS * (d + 1)]


def join_lines(got_ref, at):
    return jnp.concatenate([got_ref[d, pl.ds(at, COLS), :] for d in range(GROUPS)], axis=0).T


def row(ref, at):
    return ref[pl.ds(at, 1), :]


def tile(ref, at):
    return ref[pl.ds(at, 8), :]


def strided(ref, at, stride):
    return ref[pl.ds(at, 8, stride=stride), :] if stride > 1 else tile(ref, at)


def along(value, lanes):
    rows = value.shape[0]
    value, lanes = jnp.broadcast_to(value, (8, LANES)), jnp.broadcast_to(lanes, (8, LANES))
    return jnp.take_along_axis(value, lanes, axis=1, mode="promise_in_bounds")[:rows]


def pack_kernel(
    coef_in, face_in, cell_in, time_in, couple_in, rhs_in, out_ref, couple_ref, rhs_ref,
    coef_ref, face_ref, cell_ref, time_ref, skew_ref, stage, sems,
):
    pairs = (
        (cell_in, cell_ref), (face_in, face_ref), (time_in, time_ref), (couple_in, couple_ref),
        (rhs_in, rhs_ref), (coef_in, coef_ref),
    )
    copies = [pltpu.make_async_copy(a, b, sems.at[n]) for n, (a, b) in enumerate(pairs)]
    for copy in copies:
        copy.start()
    copies[0].wait()
    for i in range(WIDTH):
        for j in range(i + 1, WIDTH):
            skew_ref[skew_tile(i, j)] = cell_ref[WIDTH * i + j] - cell_ref[WIDTH * j + i]
    for copy in copies[1:]:
        copy.wait()
    pieces = []
    tails = 0
    for ref in (face_ref, skew_ref, time_ref, rhs_ref, couple_ref, coef_ref):
        rows = ref.size // LANES
        flat = ref if len(ref.shape) == 2 else ref.reshape(rows, LANES)
        for at in range(0, rows - 7, 8):
            pieces.append((flat, at))
        if rows % 8:
            stage[pl.ds(8 * tails, 8), :] = jnp.zeros((8, LANES), FP)
            stage[pl.ds(8 * tails, rows % 8), :] = flat[pl.ds(rows - rows % 8, rows % 8), :]
            pieces.append((stage, 8 * tails))
            tails += 1
    zeros = jnp.zeros((8, LANES), FP)
    for g in range(MATRIX_BLOCKS):
        part = pieces[16 * g : 16 * g + 16]
        split_lines([tile(*p) for p in part] + [zeros] * (16 - len(part)), out_ref, COLS * g)


def right_kernel(
    start_ref, low_ref, high_ref, index_ref, from_ref, couple_ref, rhs_ref, _, out_ref, stage, sem,
):
    start, low, high, rhs = [ref.reshape(4 * WIDTH, LANES) for ref in (start_ref, low_ref, high_ref, rhs_ref)]
    couple = couple_ref.reshape(16 * WIDTH, LANES)
    ids = sub_ids(8)
    lanes = [jnp.broadcast_to(index_ref[pl.ds(n, 1), :], (8, LANES)) for n in range(4)]
    kinds = [jnp.broadcast_to(from_ref[pl.ds(n, 1), :], (8, LANES)) for n in range(4)]

    def total(load, weight):
        value = load(rhs)
        sources = [load(ref) for ref in (start, low, high)]
        for n in range(4):
            got = jnp.zeros((8, LANES), FP)
            for d, source in enumerate(sources):
                got = jnp.where(kinds[n] == d, along(source, lanes[n]), got)
            value = value + weight(n) * got
        return value

    regs = []
    for c in range(4):
        for h in range(2):
            regs.append(total(
                lambda ref: strided(ref, 32 * h + c, 4),
                lambda n: strided(couple, (17 * c + 8 * h) * 4 + n, 4),
            ))

    def last_weight(n):
        value = jnp.zeros((8, LANES), FP)
        for c in range(4):
            value = jnp.where(ids == 4 + c, row(couple, (17 * c + 16) * 4 + n), value)
        return value

    regs.append(total(lambda ref: tile(ref, 60), last_weight))
    split_lines(regs + [jnp.zeros((8, LANES), FP)] * 7, stage, 0)
    copy = pltpu.make_async_copy(stage, out_ref.at[:, pl.ds(COLS * MATRIX_BLOCKS, COLS), :], sem)
    copy.start()
    copy.wait()


def left_at(j):
    return j if j < 16 else 32


def right_at(j):
    return 16 + j if j < 16 else 33


def invert_in_place(refs):
    ids = sub_ids(8)
    for k in range(WIDTH):
        for ref, base in refs:
            pivot = jnp.broadcast_to(1.0 / row(ref, base + 24 * k + k), (8, LANES))
            scaled = [tile(ref, base + 24 * k + 8 * v) * pivot for v in range(3)]
            here = ids == k % 8
            scaled[k // 8] = jnp.where(here, pivot, scaled[k // 8])
            for i in range(WIDTH):
                if i == k:
                    continue
                factor = row(ref, base + 24 * i + k)
                for v in range(3):
                    old = tile(ref, base + 24 * i + 8 * v)
                    if v == k // 8:
                        old = jnp.where(here, 0.0, old)
                    ref[pl.ds(base + 24 * i + 8 * v, 8), :] = old - factor * scaled[v]
            for v in range(3):
                ref[pl.ds(base + 24 * k + 8 * v, 8), :] = scaled[v]


def by_rows(step):
    lax.fori_loop(0, WIDTH // 2, lambda t, _: step([2 * t, 2 * t + 1]), 0)
    step([WIDTH - 1])


def plus(total, term):
    return term if total is None else total + term


def normalise(inverse, inverse_base, source, source_base, result, result_base):
    def step(rows):
        starts = [pl.multiple_of(24 * i, 8) for i in rows]
        sums = [[None] * 5 for _ in rows]
        for j in range(WIDTH):
            factors = [row(inverse, inverse_base + at + j) for at in starts]
            for v in range(5):
                value = tile(source, source_base + 40 * j + 8 * v)
                for r, factor in enumerate(factors):
                    sums[r][v] = plus(sums[r][v], factor * value)
        for r, i in enumerate(rows):
            to = pl.multiple_of(40 * i, 8)
            for v in range(5):
                result[pl.ds(result_base + to + 8 * v, 8), :] = sums[r][v]
        return 0

    by_rows(step)


def eliminate(blocks, base, diag, diag_base, low, low_base, high, high_base, new, new_base, new_diag, new_diag_base):
    ids = sub_ids(8)

    def step(rows):
        starts = [pl.multiple_of(40 * i, 8) for i in rows]
        firsts = [[None] * 5 for _ in rows]
        seconds = [[None] * 5 for _ in rows]
        for j in range(WIDTH):
            below = [row(blocks, base + at + left_at(j)) for at in starts]
            above = [row(blocks, base + at + right_at(j)) for at in starts]
            for v in range(5):
                value = tile(low, low_base + 40 * j + 8 * v)
                for r, factor in enumerate(below):
                    firsts[r][v] = plus(firsts[r][v], factor * value)
                value = tile(high, high_base + 40 * j + 8 * v)
                for r, factor in enumerate(above):
                    seconds[r][v] = plus(seconds[r][v], factor * value)
        for at, i, first, second in zip(starts, rows, firsts, seconds):
            for v in range(2):
                new[pl.ds(new_base + at + 8 * v, 8), :] = -first[v]
                new[pl.ds(new_base + at + 16 + 8 * v, 8), :] = -second[2 + v]
            rest = tile(blocks, base + at + 32) - first[4] - second[4]
            rest = jnp.where(ids == 0, -first[4], jnp.where(ids == 1, -second[4], rest))
            new[pl.ds(new_base + at + 32, 8), :] = rest
            to = pl.multiple_of(24 * i, 8)
            for v in range(2):
                new_diag[pl.ds(new_diag_base + to + 8 * v, 8), :] = (
                    tile(diag, diag_base + to + 8 * v) - first[2 + v] - second[v]
                )
            new_diag[pl.ds(new_diag_base + to + 16, 8), :] = (
                tile(diag, diag_base + to + 16) - pltpu.roll(first[4], 7, 0) - second[4]
            )
        return 0

    by_rows(step)


def matvec(ref, base, stride, at, value_row):
    sums = [None] * 3
    for j in range(WIDTH):
        value = value_row(j)
        here = at(j)
        for h in range(2):
            term = strided(ref, base + 8 * h * stride + here, stride) * value
            sums[h] = term if j == 0 else sums[h] + term
        term = row(ref, base + 16 * stride + here) * value
        sums[2] = term if j == 0 else sums[2] + term
    return sums


def minus(a, b):
    return [x - y for x, y in zip(a, b)]


def plain(j):
    return j


def vector_of(ref, base, last):
    return [tile(ref, base), tile(ref, base + 8), row(ref, last)]


def put_vector(ref, base, last, value):
    ref[pl.ds(base, 8), :] = value[0]
    ref[pl.ds(base + 8, 8), :] = value[1]
    ref[pl.ds(last, 1), :] = value[2]


def moved(value, steps):
    return [pltpu.roll(x, (COLS * steps) % LANES, 1) for x in value]


class Scratch:
    def __init__(self, ref):
        self.ref, self.next = ref, 0

    def hold(self, value):
        base = 24 * self.next
        self.next += 1
        put_vector(self.ref, base, base + 16, value)
        return lambda j: row(self.ref, base + j)


def back_substitute(held, scratch, top, forward):
    below = scratch.hold(moved(top, 1))
    own = scratch.hold(top)

    def part(index, low, high):
        base = index * BROWS
        value = minus(forward[index], matvec(held, base, 40, left_at, low))
        return minus(value, matvec(held, base, 40, right_at, high))

    one = part(2, below, own)
    one_rows = scratch.hold(one)
    return [part(0, below, one_rows), one, part(1, one_rows, own), top]


def put_cells(ref, cells, copies):
    for c in range(4):
        for d in range(copies):
            for h in range(2):
                ref[d, pl.ds(16 * c + 8 * h, 8), :] = cells[c][h]
            ref[d, pl.ds(64 + c, 1), :] = cells[c][2]
    for d in range(copies):
        ref[d, pl.ds(68, 4), :] = jnp.zeros((4, LANES), FP)


def factor_kernel(
    got_ref, wall_ref, solved_ref, inverse_ref, blocks_ref, held_ref, vectors_ref,
    stage_tiles, turned_tiles, skew_tiles, below, work_blocks, work_diag, low, high, scratch_ref,
):
    stage = stage_tiles.reshape(TOTALROWS, LANES)
    turned = turned_tiles.reshape(4 * WIDTH * WIDTH, LANES)
    skew = skew_tiles.reshape(4 * WIDTH * WIDTH, LANES)
    groups = lane_ids(1) // COLS
    for g in range(MATRIX_BLOCKS + 1):
        stage[pl.ds(128 * g, 128), :] = join_lines(got_ref, COLS * g)
    for i in range(WIDTH):
        skew_tiles[WIDTH * i + i] = jnp.zeros((4, LANES), FP)
        for j in range(WIDTH):
            turned_tiles[WIDTH * i + j] = stage_tiles[WIDTH * j + i]
            if j > i:
                value = stage_tiles[SKEW_AT // 4 + skew_tile(i, j)]
                skew_tiles[WIDTH * i + j] = value
                skew_tiles[WIDTH * j + i] = -value
    for c in range(4):
        for piece in range(5):
            at, step = (RHS_AT + c, 4) if piece == 0 else (COUPLE_AT + 68 * c + piece - 1, 4)
            for h in range(2):
                vectors_ref[pl.ds(VROWS * piece + 16 * c + 8 * h, 8), :] = strided(stage, at + 32 * h, step)
            vectors_ref[pl.ds(VROWS * piece + 64 + c, 1), :] = row(stage, at + 64)
    for piece in range(5):
        vectors_ref[pl.ds(VROWS * piece + 68, 4), :] = jnp.zeros((4, LANES), FP)
    has_below = jnp.where(groups == 0, 0.0, 1.0)
    has_above = jnp.where(groups == GROUPS - 1, 0.0, 1.0)
    for i in range(WIDTH):
        for h in range(2):
            value = strided(turned, 4 * (17 * i + 8 * h) + 3, 4)
            below[pl.ds(17 * i + 8 * h, 8), :] = pltpu.roll(value, COLS, 1) * has_below
    for i in range(0, WIDTH, 8):
        if i < 16:
            value = strided(turned, 4 * (17 * i + 16) + 3, 68)
            below[pl.ds(17 * i + 16, 8, stride=17), :] = pltpu.roll(value, COLS, 1) * has_below
    for at, source in ((288, 4 * 288 + 3), (289, COEF_AT + 3)):
        value = jnp.broadcast_to(row(stage, source), (8, LANES))
        below[pl.ds(at, 1), :] = (pltpu.roll(value, COLS, 1) * has_below)[:1]
    wall = jnp.zeros((1, LANES), FP)
    for kind, level in enumerate(WALLS):
        wall = wall + jnp.where(wall_ref[...] == kind, level, 0.0)
    ids = sub_ids(8)

    def build(c, blocks, blocks_base, diag, diag_base):
        lower, scale, shift = (below, 1, 0) if c == 0 else (turned, 4, c - 1)
        coef_low = row(below, 289) if c == 0 else row(stage, COEF_AT + c - 1)
        coef_up = row(stage, COEF_AT + c)
        on_diag = coef_low + coef_up
        if c == 0:
            on_diag = on_diag + wall * (1.0 - has_below)
        keep = has_above if c == 3 else None

        def up(value):
            return value if keep is None else value * keep

        def at(i, j):
            return 4 * (17 * i + j) + c

        def lower_at(i, j):
            return scale * (17 * i + j) + shift

        for i in range(WIDTH):
            extra = on_diag + row(stage, TIME_AT + 4 * i + c)
            for n in range(4):
                extra = extra + row(stage, COUPLE_AT + 68 * c + 4 * i + n)
            for h in range(2):
                down = -strided(lower, lower_at(i, 8 * h), scale)
                entry = strided(skew, at(i, 8 * h), 4)
                face = strided(stage, at(i, 8 * h), 4)
                if i // 8 == h:
                    here = ids == i % 8
                    entry = entry + jnp.where(here, extra, 0.0)
                    face = face - jnp.where(here, coef_up, 0.0)
                    down = down - jnp.where(here, coef_low, 0.0)
                diag[pl.ds(diag_base + 24 * i + 8 * h, 8), :] = entry
                blocks[pl.ds(blocks_base + 40 * i + 8 * h, 8), :] = down
                blocks[pl.ds(blocks_base + 40 * i + 16 + 8 * h, 8), :] = up(face)
            side = -row(lower, lower_at(i, 16))
            face = row(stage, at(i, 16))
            if i < 16:
                corner = row(skew, at(i, 16))
            else:
                corner, side, face = extra, side - coef_low, face - coef_up
            value = row(stage, RIGHT_AT + (16 * c + i if i < 16 else 68 + c))
            packed = jnp.where(ids == 0, side, jnp.where(ids == 1, up(face), jnp.where(ids == 2, value, 0.0)))
            blocks[pl.ds(blocks_base + 40 * i + 32, 8), :] = packed
            diag[pl.ds(diag_base + 24 * i + 16, 8), :] = jnp.where(ids == 0, corner, 0.0)

    B, D = BROWS, DROWS
    build(0, work_blocks, 0, inverse_ref, 0)
    build(2, work_blocks, B, inverse_ref, D)
    build(1, blocks_ref, 0, work_diag, 0)
    build(3, blocks_ref, B, work_diag, D)
    invert_in_place([(inverse_ref, 0), (inverse_ref, D)])
    normalise(inverse_ref, 0, work_blocks, 0, held_ref, 0)
    normalise(inverse_ref, D, work_blocks, B, held_ref, B)

    def turn(source, source_base, result, steps):
        for t in range(BROWS // 8):
            result[pl.ds(8 * t, 8), :] = pltpu.roll(
                tile(source, source_base + 8 * t), (COLS * steps) % LANES, 1
            )

    turn(held_ref, 0, high, -1)
    eliminate(blocks_ref, 0, work_diag, 0, held_ref, 0, held_ref, B, work_blocks, 0, inverse_ref, 2 * D)
    eliminate(blocks_ref, B, work_diag, D, held_ref, B, high, 0, blocks_ref, 2 * B, work_diag, 0)
    invert_in_place([(inverse_ref, 2 * D)])
    normalise(inverse_ref, 2 * D, work_blocks, 0, held_ref, 2 * B)
    turn(held_ref, 2 * B, high, -1)
    eliminate(
        blocks_ref, 2 * B, work_diag, 0, held_ref, 2 * B, high, 0, blocks_ref, 3 * B, inverse_ref, 3 * D
    )
    for k in range(3):
        source = 3 + k
        work_diag[pl.ds(0, D), :] = inverse_ref[pl.ds(source * D, D), :]
        invert_in_place([(inverse_ref, source * D)])
        normalise(inverse_ref, source * D, blocks_ref, source * B, work_blocks, 0)
        turn(work_blocks, 0, low, 2**k)
        turn(work_blocks, 0, high, -(2**k))
        if k < 2:
            new, new_base = blocks_ref, (source + 1) * B
        else:
            new, new_base = work_blocks, B
        eliminate(
            blocks_ref, source * B, work_diag, 0, low, 0, high, 0, new, new_base, inverse_ref, (source + 1) * D
        )
    invert_in_place([(inverse_ref, 6 * D)])
    scratch = Scratch(scratch_ref)
    last = matvec(inverse_ref, 6 * D, 24, plain, lambda j: row(work_blocks, B + 40 * j + 34))
    forward = []
    for index in range(3):
        base = index * B
        forward.append([
            strided(held_ref, base + 34, 40),
            strided(held_ref, base + 320 + 34, 40),
            row(held_ref, base + 640 + 34),
        ])
    put_cells(solved_ref, back_substitute(held_ref, scratch, last, forward), GROUPS)


def solve_kernel(
    all_ref, low_ref, high_ref, index_ref, from_ref, vectors_ref, inverse_ref, blocks_ref, held_ref,
    out_ref, right, scratch_ref,
):
    for t in range(VROWS // 8):
        at = 8 * t
        total = tile(vectors_ref, at)
        for n in range(4):
            lanes = jnp.broadcast_to(index_ref[pl.ds(n, 1), :], (8, LANES))
            source = jnp.broadcast_to(from_ref[pl.ds(n, 1), :], (8, LANES))
            value = jnp.zeros((8, LANES), FP)
            for d in range(GROUPS + 2):
                if d < GROUPS:
                    got = all_ref[d, pl.ds(at, 8), :]
                else:
                    got = tile(low_ref if d == GROUPS else high_ref, at)
                value = jnp.where(source == d, along(got, lanes), value)
            total = total + tile(vectors_ref, VROWS * (n + 1) + at) * value
        right[pl.ds(at, 8), :] = total
    B, D = BROWS, DROWS
    scratch = Scratch(scratch_ref)

    def cell_rows(c):
        return lambda j: row(right, 16 * c + j if j < 16 else 64 + c)

    def cell(c):
        return vector_of(right, 16 * c, 64 + c)

    def apply(index, rows):
        return matvec(inverse_ref, index * D, 24, plain, rows)

    def reduce(value, index, low, high):
        value = minus(value, matvec(blocks_ref, index * B, 40, left_at, low))
        return minus(value, matvec(blocks_ref, index * B, 40, right_at, high))

    zero = apply(0, cell_rows(0))
    two = apply(1, cell_rows(2))
    zero_rows, two_rows = scratch.hold(zero), scratch.hold(two)
    next_zero = scratch.hold(moved(zero, -1))
    one = apply(2, scratch.hold(reduce(cell(1), 0, zero_rows, two_rows)))
    three = reduce(cell(3), 1, two_rows, next_zero)
    one_rows, next_one = scratch.hold(one), scratch.hold(moved(one, -1))
    three = reduce(three, 2, one_rows, next_one)
    for k in range(3):
        scaled = apply(3 + k, scratch.hold(three))
        low, high = scratch.hold(moved(scaled, 2**k)), scratch.hold(moved(scaled, -(2**k)))
        three = reduce(three, 3 + k, low, high)
    last = apply(6, scratch.hold(three))
    cells = back_substitute(held_ref, scratch, last, [zero, two, one])
    regs = [cells[c][h] for c in range(4) for h in range(2)]
    value = jnp.zeros((8, LANES), FP)
    for c in range(4):
        value = jnp.where(sub_ids(8) == c, cells[c][2], value)
    regs.append(value)
    split_lines(regs + [jnp.zeros((8, LANES), FP)] * 7, out_ref, 0)


def unpack_kernel(got_ref, out_ref):
    flat = out_ref.reshape(4 * WIDTH, LANES)
    joined = join_lines(got_ref, 0)
    for c in range(4):
        for h in range(2):
            at = 16 * c + 8 * h
            flat[pl.ds(32 * h + c, 8, stride=4), :] = joined[at : at + 8]
    flat[pl.ds(64, 4), :] = joined[64:68]


def edge_kernel(top_ref, bottom_ref, top_out_ref, bottom_out_ref):
    top_out_ref[...] = top_ref[0]
    bottom_out_ref[...] = bottom_ref[0]


def shape(*dims):
    return jax.ShapeDtypeStruct(dims, FP)


def call(kernel, outputs, scratch, args, flops, name, limit=16, **more):
    return pl.pallas_call(
        kernel,
        out_shape=outputs,
        scratch_shapes=[pltpu.VMEM(dims, FP) if isinstance(dims, tuple) else dims for dims in scratch],
        compiler_params=pltpu.CompilerParams(vmem_limit_bytes=limit * 2**20),
        cost_estimate=pl.CostEstimate(flops=flops, bytes_accessed=1000000, transcendentals=0),
        name=name,
        **more,
    )(*args)


def across(value):
    return lax.all_to_all(value, "line", 0, 0, tiled=True)


def on_device(
    face_coef, face_mix, cell_mix, time_term, couple, rhs, start_delta, neighbours, wall_type
):
    count = lax.axis_size("surf")
    up = [(i, (i + 1) % count) for i in range(count)]
    down = [(target, source) for source, target in up]
    lines = wall_type.shape[0]
    place = lax.axis_index("line")
    start = start_delta.transpose(1, 0, 2)
    rhs_rows = rhs.transpose(1, 0, 2)
    couple_rows = couple.transpose(0, 2, 1, 3).reshape(4 * WIDTH, 4, lines)
    face, cell = [a.transpose(1, 2, 0, 3).reshape(WIDTH * WIDTH, 4, lines) for a in (face_mix, cell_mix)]
    low = lax.ppermute(start, "surf", up)
    high = lax.ppermute(start, "surf", down)

    surf_place = lax.axis_index("surf")
    local = (neighbours - (surf_place * lines - COLS)) % (lines * count)
    is_low = local < COLS
    is_own = (local >= COLS) & (local < COLS + lines)
    valid = neighbours >= 0
    own_index = jnp.clip(local - COLS, 0, lines - 1)
    kind = jnp.where(is_own, 0, jnp.where(is_low, 1, 2))
    kind = jnp.where(valid, kind, -1)
    index = jnp.where(is_own, own_index, jnp.where(is_low, local + lines - COLS, local - lines - COLS))
    index = jnp.clip(index, 0, lines - 1)
    source = jnp.where(is_own, own_index // COLS, jnp.where(is_low, GROUPS, GROUPS + 1))
    source = jnp.where(valid, source, -1)
    offset = index % COLS

    def for_group(array):
        mine = lax.dynamic_slice_in_dim(array, place * COLS, COLS, axis=array.ndim - 1)
        return jnp.tile(mine, (1, GROUPS))

    group_offset = for_group(offset) + (jnp.arange(lines, dtype=jnp.int32) // COLS * COLS)[None]
    group_source = for_group(source)
    group_wall = for_group(wall_type[None])

    any_place = pl.BlockSpec(memory_space=pl.ANY)
    vmem = pl.BlockSpec(memory_space=pltpu.VMEM)
    packed, couple_rows, rhs_rows = call(
        pack_kernel,
        (shape(GROUPS, TOTALROWS // 8, LANES), shape(4 * WIDTH, 4, LANES), shape(WIDTH, 4, LANES)),
        [
            (4, LANES), (WIDTH * WIDTH, 4, LANES), (WIDTH * WIDTH, 4, LANES), (WIDTH, 4, LANES),
            (SKEW_TILES, 4, LANES), (40, LANES), pltpu.SemaphoreType.DMA((6,)),
        ],
        [
            pltpu.with_memory_space_constraint(a, pltpu.HBM)
            for a in (face_coef, face, cell, time_term.transpose(1, 0, 2), couple_rows, rhs_rows)
        ],
        20000000,
        "pack",
        in_specs=[pl.BlockSpec(memory_space=pltpu.HBM)] * 6,
        out_specs=(vmem,) * 3,
    )
    packed = call(
        right_kernel,
        shape(GROUPS, TOTALROWS // 8, LANES),
        [(GROUPS, COLS, LANES), pltpu.SemaphoreType.DMA(())],
        (start, low, high, index, kind, couple_rows, rhs_rows, packed),
        1000000,
        "right",
        in_specs=[pl.BlockSpec(memory_space=pltpu.VMEM)] * 7 + [any_place],
        out_specs=any_place,
        input_output_aliases={7: 0},
    )
    packed, group_offset, group_source, group_wall = lax.optimization_barrier(
        (packed, group_offset, group_source, group_wall)
    )
    received = across(packed)
    solved, inverses, blocks, held, vectors = call(
        factor_kernel,
        (
            shape(GROUPS, VROWS, LANES),
            shape(7 * DROWS, LANES),
            shape(6 * BROWS, LANES),
            shape(3 * BROWS, LANES),
            shape(5 * VROWS, LANES),
        ),
        [
            (TOTALROWS // 4, 4, LANES), (WIDTH * WIDTH, 4, LANES), (WIDTH * WIDTH, 4, LANES),
            (BELOWROWS, LANES), (2 * BROWS, LANES), (2 * DROWS, LANES),
            (BROWS, LANES), (BROWS, LANES), (24 * 4, LANES),
        ],
        (received, group_wall),
        30000000,
        "factor",
    )
    everyone = across(solved)
    top, bottom = call(
        edge_kernel, (shape(VROWS, LANES), shape(VROWS, LANES)), [], (everyone, everyone), 1000, "edge", 1,
        grid=(1,),
        in_specs=[pl.BlockSpec((1, VROWS, LANES), lambda i: (GROUPS - 1, 0, 0)), pl.BlockSpec((1, VROWS, LANES), lambda i: (0, 0, 0))],
    )
    low = lax.ppermute(top, "surf", up)
    high = lax.ppermute(bottom, "surf", down)
    sent = call(
        solve_kernel,
        shape(GROUPS, COLS, LANES),
        [(VROWS, LANES), (24 * 24, LANES)],
        (everyone, low, high, group_offset, group_source, vectors, inverses, blocks, held),
        3000000,
        "solve",
    )
    done = call(unpack_kernel, shape(WIDTH, 4, LANES), [], (across(sent),), 100000, "unpack")
    return done.transpose(1, 0, 2)


def solution(mesh):
    placed = (
        P("line", "surf"),
        P("line", None, None, "surf"),
        P("line", None, None, "surf"),
        P("line", None, "surf"),
        P("line", None, None, "surf"),
        P("line", None, "surf"),
        P("line", None, "surf"),
        P(None, "surf"),
        P("surf"),
    )
    return jax.shard_map(
        on_device, mesh=mesh, in_specs=placed, out_specs=P("line", None, "surf"), check_vma=False
    )
```

```python
import jax
import jax.numpy as jnp
from jax import lax
from jax.experimental import pallas as pl
from jax.experimental.pallas import tpu as pltpu
from jax.sharding import PartitionSpec as P

COLS = 16
WIDTH = 17
GROUPS = 8
LANES = 128
DROWS = 24 * WIDTH
BROWS = 40 * WIDTH
BELOWROWS = 296
VROWS = 72
UNROLL = True
MATRIX_BLOCKS = 17
TOTALROWS = 128 * (MATRIX_BLOCKS + 1)
SKEW_TILES = WIDTH * (WIDTH - 1) // 2
SKEW_AT = 1160
TIME_AT = SKEW_AT + 4 * SKEW_TILES
RHS_AT, COUPLE_AT = TIME_AT + 72, TIME_AT + 144
COEF_AT = COUPLE_AT + 272
RIGHT_AT = 128 * MATRIX_BLOCKS
WALLS = (0.5, 4.0, 32.0)
FP = jnp.float32


def lane_ids(rows):
    return lax.broadcasted_iota(jnp.int32, (rows, LANES), 1)


def sub_ids(rows):
    return lax.broadcasted_iota(jnp.int32, (rows, LANES), 0)


def skew_tile(i, j):
    return 16 * i - i * (i - 1) // 2 + j - i - 1


def split_lines(tiles, out_ref, at):
    turned = jnp.concatenate(tiles, axis=0).T
    for d in range(GROUPS):
        out_ref[d, pl.ds(at, COLS), :] = turned[COLS * d : COLS * (d + 1)]


def join_lines(got_ref, at):
    return jnp.concatenate([got_ref[d, pl.ds(at, COLS), :] for d in range(GROUPS)], axis=0).T


def row(ref, at):
    return ref[pl.ds(at, 1), :]


def tile(ref, at):
    return ref[pl.ds(at, 8), :]


def strided(ref, at, stride):
    return ref[pl.ds(at, 8, stride=stride), :] if stride > 1 else tile(ref, at)


def along(value, lanes):
    rows = value.shape[0]
    value, lanes = jnp.broadcast_to(value, (8, LANES)), jnp.broadcast_to(lanes, (8, LANES))
    return jnp.take_along_axis(value, lanes, axis=1, mode="promise_in_bounds")[:rows]


def pack_kernel(
    coef_in, face_in, cell_in, time_in, couple_in, rhs_in, out_ref, couple_ref, rhs_ref,
    coef_ref, face_ref, cell_ref, time_ref, skew_ref, stage, sems,
):
    pairs = (
        (cell_in, cell_ref), (face_in, face_ref), (time_in, time_ref), (couple_in, couple_ref),
        (rhs_in, rhs_ref), (coef_in, coef_ref),
    )
    copies = [pltpu.make_async_copy(a, b, sems.at[n]) for n, (a, b) in enumerate(pairs)]
    for copy in copies:
        copy.start()
    copies[0].wait()
    for i in range(WIDTH):
        for j in range(i + 1, WIDTH):
            skew_ref[skew_tile(i, j)] = cell_ref[WIDTH * i + j] - cell_ref[WIDTH * j + i]
    for copy in copies[1:]:
        copy.wait()
    pieces = []
    tails = 0
    for ref in (face_ref, skew_ref, time_ref, rhs_ref, couple_ref, coef_ref):
        rows = ref.size // LANES
        flat = ref if len(ref.shape) == 2 else ref.reshape(rows, LANES)
        for at in range(0, rows - 7, 8):
            pieces.append((flat, at))
        if rows % 8:
            stage[pl.ds(8 * tails, 8), :] = jnp.zeros((8, LANES), FP)
            stage[pl.ds(8 * tails, rows % 8), :] = flat[pl.ds(rows - rows % 8, rows % 8), :]
            pieces.append((stage, 8 * tails))
            tails += 1
    zeros = jnp.zeros((8, LANES), FP)
    for g in range(MATRIX_BLOCKS):
        part = pieces[16 * g : 16 * g + 16]
        split_lines([tile(*p) for p in part] + [zeros] * (16 - len(part)), out_ref, COLS * g)


def right_kernel(
    start_ref, low_ref, high_ref, index_ref, from_ref, couple_ref, rhs_ref, _, out_ref, stage, sem,
):
    start, low, high, rhs = [ref.reshape(4 * WIDTH, LANES) for ref in (start_ref, low_ref, high_ref, rhs_ref)]
    couple = couple_ref.reshape(16 * WIDTH, LANES)
    ids = sub_ids(8)
    lanes = [jnp.broadcast_to(index_ref[pl.ds(n, 1), :], (8, LANES)) for n in range(4)]
    kinds = [jnp.broadcast_to(from_ref[pl.ds(n, 1), :], (8, LANES)) for n in range(4)]

    def total(load, weight):
        value = load(rhs)
        sources = [load(ref) for ref in (start, low, high)]
        for n in range(4):
            got = jnp.zeros((8, LANES), FP)
            for d, source in enumerate(sources):
                got = jnp.where(kinds[n] == d, along(source, lanes[n]), got)
            value = value + weight(n) * got
        return value

    regs = []
    for c in range(4):
        for h in range(2):
            regs.append(total(
                lambda ref: strided(ref, 32 * h + c, 4),
                lambda n: strided(couple, (17 * c + 8 * h) * 4 + n, 4),
            ))

    def last_weight(n):
        value = jnp.zeros((8, LANES), FP)
        for c in range(4):
            value = jnp.where(ids == 4 + c, row(couple, (17 * c + 16) * 4 + n), value)
        return value

    regs.append(total(lambda ref: tile(ref, 60), last_weight))
    split_lines(regs + [jnp.zeros((8, LANES), FP)] * 7, stage, 0)
    copy = pltpu.make_async_copy(stage, out_ref.at[:, pl.ds(COLS * MATRIX_BLOCKS, COLS), :], sem)
    copy.start()
    copy.wait()


def left_at(j):
    return j if j < 16 else 32


def right_at(j):
    return 16 + j if j < 16 else 33


def invert_in_place(refs):
    ids = sub_ids(8)
    for k in range(WIDTH):
        for ref, base in refs:
            pivot = jnp.broadcast_to(1.0 / row(ref, base + 24 * k + k), (8, LANES))
            scaled = [tile(ref, base + 24 * k + 8 * v) * pivot for v in range(3)]
            here = ids == k % 8
            scaled[k // 8] = jnp.where(here, pivot, scaled[k // 8])
            for i in range(WIDTH):
                if i == k:
                    continue
                factor = row(ref, base + 24 * i + k)
                for v in range(3):
                    old = tile(ref, base + 24 * i + 8 * v)
                    if v == k // 8:
                        old = jnp.where(here, 0.0, old)
                    ref[pl.ds(base + 24 * i + 8 * v, 8), :] = old - factor * scaled[v]
            for v in range(3):
                ref[pl.ds(base + 24 * k + 8 * v, 8), :] = scaled[v]


def by_rows(step):
    lax.fori_loop(0, WIDTH // 2, lambda t, _: step([2 * t, 2 * t + 1]), 0, unroll=UNROLL)
    step([WIDTH - 1])


def plus(total, term):
    return term if total is None else total + term


def normalise(inverse, inverse_base, source, source_base, result, result_base, shifted=None, steps=0):
    def step(rows):
        starts = [pl.multiple_of(24 * i, 8) for i in rows]
        sums = [[None] * 5 for _ in rows]
        for j in range(WIDTH):
            factors = [row(inverse, inverse_base + at + j) for at in starts]
            for v in range(5):
                value = tile(source, source_base + 40 * j + 8 * v)
                for r, factor in enumerate(factors):
                    sums[r][v] = plus(sums[r][v], factor * value)
        for r, i in enumerate(rows):
            to = pl.multiple_of(40 * i, 8)
            for v in range(5):
                result[pl.ds(result_base + to + 8 * v, 8), :] = sums[r][v]
                if shifted is not None:
                    shifted[pl.ds(to + 8 * v, 8), :] = pltpu.roll(sums[r][v], (COLS * steps) % LANES, 1)
        return 0

    by_rows(step)


def eliminate(blocks, base, diag, diag_base, low, low_base, high, high_base, new, new_base, new_diag, new_diag_base):
    ids = sub_ids(8)

    def step(rows):
        starts = [pl.multiple_of(40 * i, 8) for i in rows]
        firsts = [[None] * 5 for _ in rows]
        seconds = [[None] * 5 for _ in rows]
        for j in range(WIDTH):
            below = [row(blocks, base + at + left_at(j)) for at in starts]
            above = [row(blocks, base + at + right_at(j)) for at in starts]
            for v in range(5):
                value = tile(low, low_base + 40 * j + 8 * v)
                for r, factor in enumerate(below):
                    firsts[r][v] = plus(firsts[r][v], factor * value)
                value = tile(high, high_base + 40 * j + 8 * v)
                for r, factor in enumerate(above):
                    seconds[r][v] = plus(seconds[r][v], factor * value)
        for at, i, first, second in zip(starts, rows, firsts, seconds):
            for v in range(2):
                new[pl.ds(new_base + at + 8 * v, 8), :] = -first[v]
                new[pl.ds(new_base + at + 16 + 8 * v, 8), :] = -second[2 + v]
            rest = tile(blocks, base + at + 32) - first[4] - second[4]
            rest = jnp.where(ids == 0, -first[4], jnp.where(ids == 1, -second[4], rest))
            new[pl.ds(new_base + at + 32, 8), :] = rest
            to = pl.multiple_of(24 * i, 8)
            for v in range(2):
                new_diag[pl.ds(new_diag_base + to + 8 * v, 8), :] = (
                    tile(diag, diag_base + to + 8 * v) - first[2 + v] - second[v]
                )
            new_diag[pl.ds(new_diag_base + to + 16, 8), :] = (
                tile(diag, diag_base + to + 16) - pltpu.roll(first[4], 7, 0) - second[4]
            )
        return 0

    by_rows(step)


def finish(blocks, base, diag, diag_base, low, high, value_ref, new_diag, new_diag_base):
    def step(rows):
        starts = [pl.multiple_of(40 * i, 8) for i in rows]
        sums = [[None] * 2 for _ in rows]
        ends = [[None] * 2 for _ in rows]
        for j in range(WIDTH):
            below = [row(blocks, base + at + left_at(j)) for at in starts]
            above = [row(blocks, base + at + right_at(j)) for at in starts]
            for v in range(2):
                first, second = tile(low, 40 * j + 16 + 8 * v), tile(high, 40 * j + 8 * v)
                for r in range(len(rows)):
                    sums[r][v] = plus(sums[r][v], below[r] * first + above[r] * second)
            first, second = tile(low, 40 * j + 32), tile(high, 40 * j + 32)
            for r in range(len(rows)):
                ends[r][0] = plus(ends[r][0], below[r] * first)
                ends[r][1] = plus(ends[r][1], above[r] * second)
        for r, (at, i) in enumerate(zip(starts, rows)):
            first, second = ends[r]
            value_ref[pl.ds(at, 8), :] = tile(blocks, base + at + 32) - first - second
            to = pl.multiple_of(24 * i, 8)
            for v in range(2):
                new_diag[pl.ds(new_diag_base + to + 8 * v, 8), :] = tile(diag, diag_base + to + 8 * v) - sums[r][v]
            new_diag[pl.ds(new_diag_base + to + 16, 8), :] = (
                tile(diag, diag_base + to + 16) - pltpu.roll(first, 7, 0) - second
            )
        return 0

    by_rows(step)


def matvec(ref, base, stride, at, value_row):
    sums = [None] * 3
    for j in range(WIDTH):
        value = value_row(j)
        here = at(j)
        for h in range(2):
            term = strided(ref, base + 8 * h * stride + here, stride) * value
            sums[h] = term if j == 0 else sums[h] + term
        term = row(ref, base + 16 * stride + here) * value
        sums[2] = term if j == 0 else sums[2] + term
    return sums


def minus(a, b):
    return [x - y for x, y in zip(a, b)]


def plain(j):
    return j


def vector_of(ref, base, last):
    return [tile(ref, base), tile(ref, base + 8), row(ref, last)]


def put_vector(ref, base, last, value):
    ref[pl.ds(base, 8), :] = value[0]
    ref[pl.ds(base + 8, 8), :] = value[1]
    ref[pl.ds(last, 1), :] = value[2]


def moved(value, steps):
    return [pltpu.roll(x, (COLS * steps) % LANES, 1) for x in value]


class Scratch:
    def __init__(self, ref):
        self.ref, self.next = ref, 0

    def hold(self, value):
        base = 24 * self.next
        self.next += 1
        put_vector(self.ref, base, base + 16, value)
        return lambda j: row(self.ref, base + j)


def back_substitute(held, scratch, top, forward):
    below = scratch.hold(moved(top, 1))
    own = scratch.hold(top)

    def part(index, low, high):
        base = index * BROWS
        value = minus(forward[index], matvec(held, base, 40, left_at, low))
        return minus(value, matvec(held, base, 40, right_at, high))

    one = part(2, below, own)
    one_rows = scratch.hold(one)
    return [part(0, below, one_rows), one, part(1, one_rows, own), top]


def put_cells(ref, cells, copies):
    for c in range(4):
        for d in range(copies):
            for h in range(2):
                ref[d, pl.ds(16 * c + 8 * h, 8), :] = cells[c][h]
            ref[d, pl.ds(64 + c, 1), :] = cells[c][2]
    for d in range(copies):
        ref[d, pl.ds(68, 4), :] = jnp.zeros((4, LANES), FP)


def factor_kernel(
    got_ref, wall_ref, solved_ref, inverse_ref, blocks_ref, held_ref, vectors_ref,
    stage_tiles, turned_tiles, skew_tiles, below, work_blocks, work_diag, low, high, scratch_ref,
):
    stage = stage_tiles.reshape(TOTALROWS, LANES)
    turned = turned_tiles.reshape(4 * WIDTH * WIDTH, LANES)
    skew = skew_tiles.reshape(4 * WIDTH * WIDTH, LANES)
    groups = lane_ids(1) // COLS
    for g in range(MATRIX_BLOCKS + 1):
        stage[pl.ds(128 * g, 128), :] = join_lines(got_ref, COLS * g)
    for i in range(WIDTH):
        skew_tiles[WIDTH * i + i] = jnp.zeros((4, LANES), FP)
        for j in range(WIDTH):
            turned_tiles[WIDTH * i + j] = stage_tiles[WIDTH * j + i]
            if j > i:
                value = stage_tiles[SKEW_AT // 4 + skew_tile(i, j)]
                skew_tiles[WIDTH * i + j] = value
                skew_tiles[WIDTH * j + i] = -value
    for c in range(4):
        for piece in range(5):
            at, step = (RHS_AT + c, 4) if piece == 0 else (COUPLE_AT + 68 * c + piece - 1, 4)
            for h in range(2):
                vectors_ref[pl.ds(VROWS * piece + 16 * c + 8 * h, 8), :] = strided(stage, at + 32 * h, step)
            vectors_ref[pl.ds(VROWS * piece + 64 + c, 1), :] = row(stage, at + 64)
    for piece in range(5):
        vectors_ref[pl.ds(VROWS * piece + 68, 4), :] = jnp.zeros((4, LANES), FP)
    has_below = jnp.where(groups == 0, 0.0, 1.0)
    has_above = jnp.where(groups == GROUPS - 1, 0.0, 1.0)
    for i in range(WIDTH):
        for h in range(2):
            value = strided(turned, 4 * (17 * i + 8 * h) + 3, 4)
            below[pl.ds(17 * i + 8 * h, 8), :] = pltpu.roll(value, COLS, 1) * has_below
    for i in range(0, WIDTH, 8):
        if i < 16:
            value = strided(turned, 4 * (17 * i + 16) + 3, 68)
            below[pl.ds(17 * i + 16, 8, stride=17), :] = pltpu.roll(value, COLS, 1) * has_below
    for at, source in ((288, 4 * 288 + 3), (289, COEF_AT + 3)):
        value = jnp.broadcast_to(row(stage, source), (8, LANES))
        below[pl.ds(at, 1), :] = (pltpu.roll(value, COLS, 1) * has_below)[:1]
    wall = jnp.zeros((1, LANES), FP)
    for kind, level in enumerate(WALLS):
        wall = wall + jnp.where(wall_ref[...] == kind, level, 0.0)
    ids = sub_ids(8)

    def build(c, blocks, blocks_base, diag, diag_base):
        lower, scale, shift = (below, 1, 0) if c == 0 else (turned, 4, c - 1)
        coef_low = row(below, 289) if c == 0 else row(stage, COEF_AT + c - 1)
        coef_up = row(stage, COEF_AT + c)
        on_diag = coef_low + coef_up
        if c == 0:
            on_diag = on_diag + wall * (1.0 - has_below)
        keep = has_above if c == 3 else None

        def up(value):
            return value if keep is None else value * keep

        def at(i, j):
            return 4 * (17 * i + j) + c

        def lower_at(i, j):
            return scale * (17 * i + j) + shift

        for i in range(WIDTH):
            extra = on_diag + row(stage, TIME_AT + 4 * i + c)
            for n in range(4):
                extra = extra + row(stage, COUPLE_AT + 68 * c + 4 * i + n)
            for h in range(2):
                down = -strided(lower, lower_at(i, 8 * h), scale)
                entry = strided(skew, at(i, 8 * h), 4)
                face = strided(stage, at(i, 8 * h), 4)
                if i // 8 == h:
                    here = ids == i % 8
                    entry = entry + jnp.where(here, extra, 0.0)
                    face = face - jnp.where(here, coef_up, 0.0)
                    down = down - jnp.where(here, coef_low, 0.0)
                diag[pl.ds(diag_base + 24 * i + 8 * h, 8), :] = entry
                blocks[pl.ds(blocks_base + 40 * i + 8 * h, 8), :] = down
                blocks[pl.ds(blocks_base + 40 * i + 16 + 8 * h, 8), :] = up(face)
            side = -row(lower, lower_at(i, 16))
            face = row(stage, at(i, 16))
            if i < 16:
                corner = row(skew, at(i, 16))
            else:
                corner, side, face = extra, side - coef_low, face - coef_up
            value = row(stage, RIGHT_AT + (16 * c + i if i < 16 else 68 + c))
            packed = jnp.where(ids == 0, side, jnp.where(ids == 1, up(face), jnp.where(ids == 2, value, 0.0)))
            blocks[pl.ds(blocks_base + 40 * i + 32, 8), :] = packed
            diag[pl.ds(diag_base + 24 * i + 16, 8), :] = jnp.where(ids == 0, corner, 0.0)

    B, D = BROWS, DROWS
    build(0, work_blocks, 0, inverse_ref, 0)
    build(2, work_blocks, B, inverse_ref, D)
    build(1, blocks_ref, 0, work_diag, 0)
    build(3, blocks_ref, B, work_diag, D)
    invert_in_place([(inverse_ref, 0), (inverse_ref, D)])
    normalise(inverse_ref, 0, work_blocks, 0, held_ref, 0, high, -1)
    normalise(inverse_ref, D, work_blocks, B, held_ref, B)

    def turn(source, source_base, result, steps):
        for t in range(BROWS // 8):
            result[pl.ds(8 * t, 8), :] = pltpu.roll(
                tile(source, source_base + 8 * t), (COLS * steps) % LANES, 1
            )

    eliminate(blocks_ref, 0, work_diag, 0, held_ref, 0, held_ref, B, work_blocks, 0, inverse_ref, 2 * D)
    eliminate(blocks_ref, B, work_diag, D, held_ref, B, high, 0, blocks_ref, 2 * B, work_diag, 0)
    invert_in_place([(inverse_ref, 2 * D)])
    normalise(inverse_ref, 2 * D, work_blocks, 0, held_ref, 2 * B, high, -1)
    eliminate(
        blocks_ref, 2 * B, work_diag, 0, held_ref, 2 * B, high, 0, blocks_ref, 3 * B, inverse_ref, 3 * D
    )
    for k in range(3):
        source = 3 + k
        work_diag[pl.ds(0, D), :] = inverse_ref[pl.ds(source * D, D), :]
        invert_in_place([(inverse_ref, source * D)])
        normalise(inverse_ref, source * D, blocks_ref, source * B, work_blocks, 0, low, 2**k)
        if k < 2:
            turn(work_blocks, 0, high, -(2**k))
            eliminate(
                blocks_ref, source * B, work_diag, 0, low, 0, high, 0, blocks_ref, (source + 1) * B,
                inverse_ref, (source + 1) * D,
            )
        else:
            finish(blocks_ref, source * B, work_diag, 0, low, low, high, inverse_ref, (source + 1) * D)
    invert_in_place([(inverse_ref, 6 * D)])
    scratch = Scratch(scratch_ref)
    last = matvec(inverse_ref, 6 * D, 24, plain, lambda j: row(high, 40 * j + 2))
    forward = []
    for index in range(3):
        base = index * B
        forward.append([
            strided(held_ref, base + 34, 40),
            strided(held_ref, base + 320 + 34, 40),
            row(held_ref, base + 640 + 34),
        ])
    put_cells(solved_ref, back_substitute(held_ref, scratch, last, forward), GROUPS)


def solve_kernel(
    all_ref, low_ref, high_ref, index_ref, from_ref, vectors_ref, inverse_ref, blocks_ref, held_ref,
    out_ref, right, scratch_ref,
):
    for t in range(VROWS // 8):
        at = 8 * t
        total = tile(vectors_ref, at)
        for n in range(4):
            lanes = jnp.broadcast_to(index_ref[pl.ds(n, 1), :], (8, LANES))
            source = jnp.broadcast_to(from_ref[pl.ds(n, 1), :], (8, LANES))
            value = jnp.zeros((8, LANES), FP)
            for d in range(GROUPS + 2):
                if d < GROUPS:
                    got = all_ref[d, pl.ds(at, 8), :]
                else:
                    got = tile(low_ref if d == GROUPS else high_ref, at)
                value = jnp.where(source == d, along(got, lanes), value)
            total = total + tile(vectors_ref, VROWS * (n + 1) + at) * value
        right[pl.ds(at, 8), :] = total
    B, D = BROWS, DROWS
    scratch = Scratch(scratch_ref)

    def cell_rows(c):
        return lambda j: row(right, 16 * c + j if j < 16 else 64 + c)

    def cell(c):
        return vector_of(right, 16 * c, 64 + c)

    def apply(index, rows):
        return matvec(inverse_ref, index * D, 24, plain, rows)

    def reduce(value, index, low, high):
        value = minus(value, matvec(blocks_ref, index * B, 40, left_at, low))
        return minus(value, matvec(blocks_ref, index * B, 40, right_at, high))

    zero = apply(0, cell_rows(0))
    two = apply(1, cell_rows(2))
    zero_rows, two_rows = scratch.hold(zero), scratch.hold(two)
    next_zero = scratch.hold(moved(zero, -1))
    one = apply(2, scratch.hold(reduce(cell(1), 0, zero_rows, two_rows)))
    three = reduce(cell(3), 1, two_rows, next_zero)
    one_rows, next_one = scratch.hold(one), scratch.hold(moved(one, -1))
    three = reduce(three, 2, one_rows, next_one)
    for k in range(3):
        scaled = apply(3 + k, scratch.hold(three))
        low, high = scratch.hold(moved(scaled, 2**k)), scratch.hold(moved(scaled, -(2**k)))
        three = reduce(three, 3 + k, low, high)
    last = apply(6, scratch.hold(three))
    cells = back_substitute(held_ref, scratch, last, [zero, two, one])
    regs = [cells[c][h] for c in range(4) for h in range(2)]
    value = jnp.zeros((8, LANES), FP)
    for c in range(4):
        value = jnp.where(sub_ids(8) == c, cells[c][2], value)
    regs.append(value)
    split_lines(regs + [jnp.zeros((8, LANES), FP)] * 7, out_ref, 0)


def unpack_kernel(got_ref, out_ref):
    flat = out_ref.reshape(4 * WIDTH, LANES)
    joined = join_lines(got_ref, 0)
    for c in range(4):
        for h in range(2):
            at = 16 * c + 8 * h
            flat[pl.ds(32 * h + c, 8, stride=4), :] = joined[at : at + 8]
    flat[pl.ds(64, 4), :] = joined[64:68]


def edge_kernel(top_ref, bottom_ref, top_out_ref, bottom_out_ref):
    top_out_ref[...] = top_ref[0]
    bottom_out_ref[...] = bottom_ref[0]


def shape(*dims):
    return jax.ShapeDtypeStruct(dims, FP)


def call(kernel, outputs, scratch, args, flops, name, limit=16, **more):
    return pl.pallas_call(
        kernel,
        out_shape=outputs,
        scratch_shapes=[pltpu.VMEM(dims, FP) if isinstance(dims, tuple) else dims for dims in scratch],
        compiler_params=pltpu.CompilerParams(vmem_limit_bytes=limit * 2**20),
        cost_estimate=pl.CostEstimate(flops=flops, bytes_accessed=1000000, transcendentals=0),
        name=name,
        **more,
    )(*args)


def across(value):
    return lax.all_to_all(value, "line", 0, 0, tiled=True)


def on_device(
    face_coef, face_mix, cell_mix, time_term, couple, rhs, start_delta, neighbours, wall_type
):
    count = lax.axis_size("surf")
    up = [(i, (i + 1) % count) for i in range(count)]
    down = [(target, source) for source, target in up]
    lines = wall_type.shape[0]
    place = lax.axis_index("line")
    start = start_delta.transpose(1, 0, 2)
    rhs_rows = rhs.transpose(1, 0, 2)
    couple_rows = couple.transpose(0, 2, 1, 3).reshape(4 * WIDTH, 4, lines)
    face, cell = [a.transpose(1, 2, 0, 3).reshape(WIDTH * WIDTH, 4, lines) for a in (face_mix, cell_mix)]
    low = lax.ppermute(start, "surf", up)
    high = lax.ppermute(start, "surf", down)

    surf_place = lax.axis_index("surf")
    local = (neighbours - (surf_place * lines - COLS)) % (lines * count)
    is_low = local < COLS
    is_own = (local >= COLS) & (local < COLS + lines)
    valid = neighbours >= 0
    own_index = jnp.clip(local - COLS, 0, lines - 1)
    kind = jnp.where(is_own, 0, jnp.where(is_low, 1, 2))
    kind = jnp.where(valid, kind, -1)
    index = jnp.where(is_own, own_index, jnp.where(is_low, local + lines - COLS, local - lines - COLS))
    index = jnp.clip(index, 0, lines - 1)
    source = jnp.where(is_own, own_index // COLS, jnp.where(is_low, GROUPS, GROUPS + 1))
    source = jnp.where(valid, source, -1)
    offset = index % COLS

    def for_group(array):
        mine = lax.dynamic_slice_in_dim(array, place * COLS, COLS, axis=array.ndim - 1)
        return jnp.tile(mine, (1, GROUPS))

    group_offset = for_group(offset) + (jnp.arange(lines, dtype=jnp.int32) // COLS * COLS)[None]
    group_source = for_group(source)
    group_wall = for_group(wall_type[None])

    any_place = pl.BlockSpec(memory_space=pl.ANY)
    vmem = pl.BlockSpec(memory_space=pltpu.VMEM)
    packed, couple_rows, rhs_rows = call(
        pack_kernel,
        (shape(GROUPS, TOTALROWS // 8, LANES), shape(4 * WIDTH, 4, LANES), shape(WIDTH, 4, LANES)),
        [
            (4, LANES), (WIDTH * WIDTH, 4, LANES), (WIDTH * WIDTH, 4, LANES), (WIDTH, 4, LANES),
            (SKEW_TILES, 4, LANES), (40, LANES), pltpu.SemaphoreType.DMA((6,)),
        ],
        [
            pltpu.with_memory_space_constraint(a, pltpu.HBM)
            for a in (face_coef, face, cell, time_term.transpose(1, 0, 2), couple_rows, rhs_rows)
        ],
        20000000,
        "pack",
        in_specs=[pl.BlockSpec(memory_space=pltpu.HBM)] * 6,
        out_specs=(vmem,) * 3,
    )
    packed = call(
        right_kernel,
        shape(GROUPS, TOTALROWS // 8, LANES),
        [(GROUPS, COLS, LANES), pltpu.SemaphoreType.DMA(())],
        (start, low, high, index, kind, couple_rows, rhs_rows, packed),
        1000000,
        "right",
        in_specs=[pl.BlockSpec(memory_space=pltpu.VMEM)] * 7 + [any_place],
        out_specs=any_place,
        input_output_aliases={7: 0},
    )
    packed, group_offset, group_source, group_wall = lax.optimization_barrier(
        (packed, group_offset, group_source, group_wall)
    )
    received = across(packed)
    solved, inverses, blocks, held, vectors = call(
        factor_kernel,
        (
            shape(GROUPS, VROWS, LANES),
            shape(7 * DROWS, LANES),
            shape(6 * BROWS, LANES),
            shape(3 * BROWS, LANES),
            shape(5 * VROWS, LANES),
        ),
        [
            (TOTALROWS // 4, 4, LANES), (WIDTH * WIDTH, 4, LANES), (WIDTH * WIDTH, 4, LANES),
            (BELOWROWS, LANES), (2 * BROWS, LANES), (2 * DROWS, LANES),
            (BROWS, LANES), (BROWS, LANES), (24 * 4, LANES),
        ],
        (received, group_wall),
        30000000,
        "factor",
    )
    everyone = across(solved)
    top, bottom = call(
        edge_kernel, (shape(VROWS, LANES), shape(VROWS, LANES)), [], (everyone, everyone), 1000, "edge", 1,
        grid=(1,),
        in_specs=[pl.BlockSpec((1, VROWS, LANES), lambda i: (GROUPS - 1, 0, 0)), pl.BlockSpec((1, VROWS, LANES), lambda i: (0, 0, 0))],
    )
    low = lax.ppermute(top, "surf", up)
    high = lax.ppermute(bottom, "surf", down)
    sent = call(
        solve_kernel,
        shape(GROUPS, COLS, LANES),
        [(VROWS, LANES), (24 * 24, LANES)],
        (everyone, low, high, group_offset, group_source, vectors, inverses, blocks, held),
        3000000,
        "solve",
    )
    done = call(unpack_kernel, shape(WIDTH, 4, LANES), [], (across(sent),), 100000, "unpack")
    return done.transpose(1, 0, 2)


def solution(mesh):
    placed = (
        P("line", "surf"),
        P("line", None, None, "surf"),
        P("line", None, None, "surf"),
        P("line", None, "surf"),
        P("line", None, None, "surf"),
        P("line", None, "surf"),
        P("line", None, "surf"),
        P(None, "surf"),
        P("surf"),
    )
    return jax.shard_map(
        on_device, mesh=mesh, in_specs=placed, out_specs=P("line", None, "surf"), check_vma=False
    )
```
